32 devices in a mesh: groups: 2 (over x), az: 16 (over z, y, core).
Axes of the slice: x: 2, y: 2, z: 4, core: 2. Of those that a mesh axis runs over, the one named last changes fastest.
Arguments:
- density: float32 [2, 4096, 1024], P('groups', 'az'), parts along dimension 0, may hold values from 0.5 to 2
- mom_radial: float32 [2, 4096, 1024], P('groups', 'az'), parts along dimension 0, may hold values from -3 to 3
- mom_azimuth: float32 [2, 4096, 1024], P('groups', 'az'), parts along dimension 0, may hold values from -3 to 3
- energy: float32 [2, 4096, 1024], P('groups', 'az'), parts along dimension 0, may hold values from 0.5 to 2
- dust: float32 [2, 4096, 1024], P('groups', 'az'), parts along dimension 0, may hold values from 0.1 to 1
- shifts: int32 [2048], P('groups'), parts along dimension 0, may hold values from 0 to 4095
- green: bfloat16 [256, 1024, 1024], P('az'), may hold values from -0.1875 to 0.1875
Outputs:
- density_out: float32 [2, 4096, 1024], P('groups', 'az'), parts along dimension 0
- mom_radial_out: float32 [2, 4096, 1024], P('groups', 'az'), parts along dimension 0
- mom_azimuth_out: float32 [2, 4096, 1024], P('groups', 'az'), parts along dimension 0
- energy_out: float32 [2, 4096, 1024], P('groups', 'az'), parts along dimension 0
- dust_out: float32 [2, 4096, 1024], P('groups', 'az'), parts along dimension 0
The draws below stay inside these ranges and needn't reach their ends.
There are 2 independent parts, one for each index of `groups`. The reference program is written for one: setup_inputs(seed, part) draws one part's arguments, and reference() takes and returns one part's arrays. A program takes and returns all parts, laid end to end along the dimension named above; an argument that names none is the same for every part. Nothing has to cross between parts.
Inputs may be any that keep to these rules, and one draw needn't show every extreme that they name: shifts[r] is the whole number of azimuthal cells that radius r moves with the mean orbital flow.
All inputs are finite; a program needn't handle non-finite values.
Results may differ from the reference program's by a relative error of at most 0.0024.
Values may be sent and summed in bfloat16 or wider, within the bound.
No kernel may reach another device: no remote copies, remote signals or barrier semaphores. Data moves between devices by JAX's collectives and lax.ppermute only.
A program may use at most 128 MiB of HBM per device.

```python
import math
import jax
import jax.numpy as jnp
from jax import lax

NR = 1024
NPHI = 4096
MODES = 256
LAYERS = 1


def plant(values, key, smallest, high):
    index_at = [jax.random.randint(jax.random.fold_in(key, axis), (), 0, length) for axis, length in enumerate(values.shape)]
    main_axis = values.shape.index(max(values.shape))
    beside = index_at[:main_axis] + [(index_at[main_axis] + 1) % values.shape[main_axis]] + index_at[main_axis + 1:]
    return values.at[tuple(index_at)].set(smallest).at[tuple(beside)].set(high)


def level_of(stream_key, dims, pieces, smallest, top_value):
    gain = 1.0
    for dim, blocks in pieces:
        heights = jax.random.uniform(jax.random.fold_in(jax.random.fold_in(stream_key, 6), dim), (blocks,), jnp.float32, smallest / len(pieces), top_value / len(pieces))
        gain = gain * jnp.repeat(jnp.exp(heights), dims[dim] // blocks).reshape((-1,) + (1,) * (len(dims) - 1 - dim))
    return gain


def normal_values(own_key, shape, deviation, reach, split=(), held_as=jnp.bfloat16):
    gain = level_of(own_key, shape, split, -0.22, 0.18) if split else 1.0
    drawn = jax.random.normal(own_key, shape, jnp.float32) * deviation * gain
    return jnp.minimum(jnp.maximum(drawn, -reach), reach).astype(held_as)


def setup_inputs(seed: int = 0, part: int = 0) -> dict:
    seeds = jax.random.split(jax.random.key(seed), 8)
    own_keys = jax.random.split(jax.random.fold_in(seeds[7], part), 8)
    return {
        "density": jnp.clip(jnp.exp(math.log(2.0) - 1.3862944 * jax.random.uniform(own_keys[0], (LAYERS, NPHI, NR), jnp.float32) ** level_of(own_keys[0], (LAYERS, NPHI, NR), ((1, 16),), -0.2, 0.2)), 0.5, 2.0),
        "mom_radial": normal_values(own_keys[1], (LAYERS, NPHI, NR), 0.2, 3.0, ((1, 16),), jnp.float32),
        "mom_azimuth": normal_values(own_keys[2], (LAYERS, NPHI, NR), 0.2, 3.0, ((1, 16),), jnp.float32),
        "energy": jnp.clip(jnp.exp(math.log(2.0) - 1.3862944 * jax.random.uniform(own_keys[3], (LAYERS, NPHI, NR), jnp.float32) ** level_of(own_keys[3], (LAYERS, NPHI, NR), ((1, 16),), -0.2, 0.2)), 0.5, 2.0),
        "dust": jnp.clip(jnp.exp(math.log(1.0) - 2.3025851 * jax.random.uniform(own_keys[4], (LAYERS, NPHI, NR), jnp.float32) ** level_of(own_keys[4], (LAYERS, NPHI, NR), ((1, 16),), -0.2, 0.2)), 0.1, 1.0),
        "shifts": plant(jax.random.randint(own_keys[5], (NR,), 0, NPHI), jax.random.fold_in(own_keys[5], 1), 0, NPHI - 1).astype(jnp.int32),
        "green": normal_values(seeds[6], (MODES, NR, NR), NR ** -0.5, 0.1875, ((0, 16),)),
    }


courant = 0.05
sound_sq = 1.0
kick_radial = 0.1
kick_azimuth = 3.0

def minmod(first_arg, second_arg):
    return 0.5 * (jnp.sign(first_arg) + jnp.sign(second_arg)) * jnp.minimum(jnp.abs(first_arg), jnp.abs(second_arg))

def trimmed(values, low_cut, high_cut, sweep_axis):
    return lax.slice_in_dim(values, low_cut, values.shape[sweep_axis] - high_cut, axis=sweep_axis)

def fluxes(state, normal, across):
    density_now = state[0]
    velocity = state[normal] / density_now
    parts = [None, None, None, None, None]
    parts[0] = state[normal]
    parts[normal] = state[normal] * velocity + sound_sq * density_now
    parts[across] = state[across] * velocity
    parts[3] = state[3] * velocity
    parts[4] = state[4] * velocity
    return (jnp.stack(parts), velocity)

def sweep_cells(padded, sweep_axis, normal, across):
    interface = 7.0 / 12.0 * (trimmed(padded, 1, 2, sweep_axis) + trimmed(padded, 2, 1, sweep_axis)) - 1.0 / 12.0 * (trimmed(padded, 0, 3, sweep_axis) + trimmed(padded, 3, 0, sweep_axis))
    centre = trimmed(padded, 2, 2, sweep_axis)
    next_cell = trimmed(padded, 3, 1, sweep_axis)
    prev_cell = trimmed(padded, 1, 3, sweep_axis)
    upper_state = centre + minmod(trimmed(interface, 1, 0, sweep_axis) - centre, next_cell - centre)
    lower_state = centre - minmod(centre - trimmed(interface, 0, 1, sweep_axis), centre - prev_cell)
    left_state = trimmed(upper_state, 0, 1, sweep_axis)
    right_state = trimmed(lower_state, 1, 0, sweep_axis)
    left_flux, left_speed = fluxes(left_state, normal, across)
    right_flux, right_speed = fluxes(right_state, normal, across)
    speeds = jnp.maximum(jnp.abs(left_speed), jnp.abs(right_speed)) + jnp.sqrt(sound_sq)
    interface_flux = 0.5 * (left_flux + right_flux) - 0.5 * speeds[None] * (right_state - left_state)
    return trimmed(padded, 3, 3, sweep_axis) - courant * (trimmed(interface_flux, 1, 0, sweep_axis) - trimmed(interface_flux, 0, 1, sweep_axis))

def green_apply(pair):
    return jnp.dot(pair[1], pair[0].T, preferred_element_type=jnp.float32)

def reference(density, mom_radial, mom_azimuth, energy, dust, shifts, green):
    state = jnp.stack([density, mom_radial, mom_azimuth, energy, dust])
    phi_ids = jnp.arange(NPHI, dtype=jnp.int32)
    source = (phi_ids[:, None] - shifts[None, :].astype(jnp.int32)) % NPHI
    state = jnp.take_along_axis(state, source[None, None, :, :], axis=2)
    padded = jnp.pad(state, ((0, 0), (0, 0), (3, 3), (0, 0)), mode='wrap')
    state = sweep_cells(padded, 2, 2, 1)
    padded = jnp.pad(state, ((0, 0), (0, 0), (0, 0), (3, 3)), mode='edge')
    state = sweep_cells(padded, 3, 1, 2)
    surface = lax.optimization_barrier(jnp.sum(state[0], axis=0))
    spectrum = jnp.fft.rfft(surface, axis=0)[:MODES]
    coeffs = jnp.stack([jnp.real(spectrum), jnp.imag(spectrum)], axis=1).astype(jnp.float32).astype(jnp.bfloat16)
    potential_modes = lax.map(green_apply, (green, coeffs)).astype(jnp.bfloat16)
    modes_float = potential_modes.astype(jnp.float32)
    complex_modes = modes_float[:, 0, :] + 1j * modes_float[:, 1, :]
    wavenum = 2.0 * jnp.pi * jnp.arange(MODES, dtype=jnp.float32) / NPHI
    potential = jnp.fft.irfft(complex_modes, n=NPHI, axis=0).astype(jnp.float32)
    slope_az = jnp.fft.irfft(1j * wavenum[:, None] * complex_modes, n=NPHI, axis=0).astype(jnp.float32)
    padded_pot = jnp.pad(potential, ((0, 0), (1, 1)), mode='edge')
    slope_r = 0.5 * (padded_pot[:, 2:] - padded_pot[:, :-2])
    mom_r_new = state[1] - kick_radial * state[0] * slope_r[None]
    mom_a_new = state[2] - kick_azimuth * state[0] * slope_az[None]
    return (state[0], mom_r_new, mom_a_new, state[3], state[4])
```

```python
import functools
import math

import jax
import jax.numpy as jnp
from jax import lax
from jax.experimental import pallas as pl
from jax.experimental.pallas import tpu as pltpu
from jax.sharding import PartitionSpec as P

courant = 0.05
kick_radial = 0.1
kick_azimuth = 3.0
FIELDS = 5
LANES = 128
HALO = 2
HALO_ROWS = 32
RANGES = ((0.5, 2.0), (-3.0, 3.0), (-3.0, 3.0), (0.5, 2.0), (0.1, 1.0))
LEVELS = tuple(0.5 * (low + high) for low, high in RANGES)
STEPS = tuple(0.5 * (high - low) / 32760.0 for low, high in RANGES)
CODE = jnp.int16
BF16 = jnp.bfloat16
F32 = jnp.float32


def vmem(count):
    return [pl.BlockSpec(memory_space=pltpu.VMEM)] * count


def pack_kernel(radii, dests, *refs):
    fields, out, halo = refs[:FIELDS], refs[FIELDS], refs[FIELDS + 1]
    total = fields[0].shape[2]
    per_tile = LANES // radii
    for f in range(FIELDS):
        for c in range(total // LANES):
            block = fields[f][0, :, c * LANES : (c + 1) * LANES].T
            block = jnp.floor((block - LEVELS[f]) * (1.0 / STEPS[f]) + 0.5)
            for k in range(per_tile):
                dest = c * per_tile + k
                own = block[k * radii : (k + 1) * radii]
                out[dest, f * radii : (f + 1) * radii, :] = own.astype(jnp.int32).astype(CODE)
                first, last = own[:HALO], own[radii - HALO :]
                row = f * 2 * HALO
                if dest > 0:
                    halo[dest - 1, row : row + HALO, :] = first
                else:
                    for i in range(HALO):
                        halo[0, row + HALO + i : row + HALO + i + 1, :] = own[:1]
                if dest < dests - 1:
                    halo[dest + 1, row + HALO : row + 2 * HALO, :] = last
                else:
                    for i in range(HALO):
                        halo[dest, row + i : row + i + 1, :] = own[radii - 1 :]
    for dest in range(dests):
        used = FIELDS * 2 * HALO
        halo[dest, used:, :] = jnp.zeros((HALO_ROWS - used, halo.shape[2]), F32)
        out[dest, FIELDS * radii :, :] = halo[dest].astype(jnp.int32).astype(CODE)


def pack(fields, radii, dests):
    width = fields[0].shape[1]
    rows = FIELDS * radii + HALO_ROWS
    return pl.pallas_call(
        functools.partial(pack_kernel, radii, dests),
        out_shape=jax.ShapeDtypeStruct((dests, rows, width), CODE),
        in_specs=vmem(FIELDS),
        out_specs=vmem(1)[0],
        scratch_shapes=[pltpu.VMEM((dests, HALO_ROWS, width), F32)],
        name="pack",
    )(*fields)


def sweep(cells, axis, normal):
    size = cells[0].shape[axis]

    def after(x):
        return pltpu.roll(x, size - 1, axis)

    def before(x):
        return pltpu.roll(x, 1, axis)

    left, right = [], []
    for q in cells:
        following = after(q)
        d = following - q
        bend = (before(d) - after(d)) * (1.0 / 12.0)
        half = 0.5 * d
        low, high = jnp.minimum(d, 0.0), jnp.maximum(d, 0.0)
        left.append(q + jnp.minimum(jnp.maximum(half + bend, low), high))
        right.append(following - jnp.minimum(jnp.maximum(half - bend, low), high))
    u_left = left[normal] / left[0]
    u_right = right[normal] / right[0]
    speed = jnp.maximum(jnp.abs(u_left), jnp.abs(u_right)) + 1.0
    w_left = 0.5 * (u_left + speed)
    w_right = 0.5 * (u_right - speed)
    swept = []
    for c, q in enumerate(cells):
        flux = left[c] * w_left + right[c] * w_right
        if c == normal:
            flux = flux + 0.5 * (left[0] + right[0])
        swept.append(q - courant * (flux - before(flux)))
    return swept


def shifted_tiles(tiles, amount):
    count = len(tiles)
    fine, coarse = amount % LANES, amount // LANES
    lane = lax.broadcasted_iota(jnp.int32, amount.shape, 1)
    index = (lane - fine) % LANES
    wraps = lane < fine
    turned = [jnp.take_along_axis(x, index, axis=1, mode="promise_in_bounds") for x in tiles]
    tiles = [jnp.where(wraps, turned[t - 1], turned[t]) for t in range(count)]
    for bit in range((count - 1).bit_length()):
        chosen = (coarse >> bit) & 1 == 1
        tiles = [jnp.where(chosen, tiles[(t - (1 << bit)) % count], tiles[t]) for t in range(count)]
    return tiles


def decoded(codes, f):
    return codes.astype(jnp.int32).astype(F32) * STEPS[f] + LEVELS[f]


def sweeps_kernel(radii, chunk, got, amounts, swept, surf, wide, turned, mid):
    sources, _, width = got.shape
    length = sources * width
    tiles = length // LANES
    blocks = radii // 8 + 1
    for f in range(FIELDS):
        for src in range(sources):
            lanes = slice(src * width, (src + 1) * width)
            wide[f, :radii, lanes] = decoded(got[src, f * radii : (f + 1) * radii, :], f)
    for src in range(sources):
        lanes = slice(src * width, (src + 1) * width)
        edge = got[src, FIELDS * radii :, :].astype(jnp.int32).astype(F32)
        for f in range(FIELDS):
            own = edge[f * 2 * HALO : (f + 1) * 2 * HALO]
            wide[f, radii : radii + 2 * HALO, lanes] = own * STEPS[f] + LEVELS[f]
            wide[f, radii + 2 * HALO :, lanes] = jnp.ones((8 - 2 * HALO, width), F32)

    def one_block(b, carry):
        rows = pl.ds(pl.multiple_of(b * 8, 8), 8)
        amount = amounts[rows, :]

        def one_field(f, carry):
            out = shifted_tiles(
                [wide[f, rows, t * LANES : (t + 1) * LANES] for t in range(tiles)], amount
            )
            for t in range(tiles):
                turned[f, :, (t + 1) * LANES : (t + 2) * LANES] = out[t]
            turned[f, :, :LANES] = out[tiles - 1]
            turned[f, :, (tiles + 1) * LANES :] = out[0]
            return carry

        lax.fori_loop(0, FIELDS, one_field, 0)

        def one_chunk(i, carry):
            start = pl.multiple_of(i * chunk, LANES)
            cells = [turned[f, :, pl.ds(start, chunk + 2 * LANES)] for f in range(FIELDS)]
            out = sweep(cells, 1, 2)
            for f in range(FIELDS):
                mid[f, pl.ds(pl.multiple_of(b * 8 + 8, 8), 8), pl.ds(start, chunk)] = out[f][
                    :, LANES : LANES + chunk
                ]
            return carry

        lax.fori_loop(0, length // chunk, one_chunk, 0)
        return carry

    lax.fori_loop(0, blocks, one_block, 0)

    def one_tile(t, carry):
        lanes = pl.ds(pl.multiple_of(t * LANES, LANES), LANES)
        for f in range(FIELDS):
            below = mid[f, radii + 8 + HALO : radii + 8 + 2 * HALO, lanes]
            mid[f, 8 - HALO : 8, lanes] = below
        cells = [mid[f, :, lanes] for f in range(FIELDS)]
        out = sweep(cells, 0, 1)
        for f in range(FIELDS):
            swept[f, :, lanes] = out[f][8 : 8 + radii]
        ripple = out[0][8 : 8 + radii] - LEVELS[0]
        high = ripple.astype(BF16)
        surf[:radii, lanes] = high
        surf[radii:, lanes] = (ripple - high.astype(F32)).astype(BF16)
        return carry

    lax.fori_loop(0, tiles, one_tile, 0)


def sweeps(got, amounts, radii):
    sources, _, width = got.shape
    length = sources * width
    chunk = min(1024, length)
    return pl.pallas_call(
        functools.partial(sweeps_kernel, radii, chunk),
        out_shape=(
            jax.ShapeDtypeStruct((FIELDS, radii, length), F32),
            jax.ShapeDtypeStruct((2 * radii, length), BF16),
        ),
        in_specs=vmem(2),
        out_specs=tuple(vmem(2)),
        scratch_shapes=[
            pltpu.VMEM((FIELDS, radii + 8, length), F32),
            pltpu.VMEM((FIELDS, 8, length + 2 * LANES), F32),
            pltpu.VMEM((FIELDS, radii + 16, length), F32),
        ],
        name="sweeps",
    )(got, amounts)


def table_kernel(outer_a, outer_b, inner_a, inner_b, out, rest):
    tiles = out.shape[1] // LANES

    def rows_at(i, carry):
        rows = pl.ds(pl.multiple_of(i * 16, 16), 16)
        a, b = inner_a[rows, :], inner_b[rows, :]
        oa, ob = outer_a[rows, :], outer_b[rows, :]
        for t in range(tiles):
            value = oa[:, t : t + 1] * a + ob[:, t : t + 1] * b
            lanes = slice(t * LANES, (t + 1) * LANES)
            high = value.astype(BF16)
            out[rows, lanes] = high
            rest[rows, lanes] = (value - high.astype(F32)).astype(BF16)
        return carry

    lax.fori_loop(0, out.shape[0] // 16, rows_at, 0)


def waves(rows, length):
    tiles = length // LANES
    row = jnp.arange(rows, dtype=jnp.int32)
    mode, odd = row // 2, (row % 2 == 1)[:, None]

    def angle(positions):
        phase = mode[:, None] * positions[None, :] % length
        return phase.astype(F32) * (2.0 * math.pi / length)

    far = angle(jnp.arange(tiles, dtype=jnp.int32) * LANES)
    near = angle(jnp.arange(LANES, dtype=jnp.int32))
    cos_far, sin_far = jnp.cos(far), jnp.sin(far)
    outer_a = jnp.where(odd, -sin_far, cos_far)
    outer_b = jnp.where(odd, -cos_far, -sin_far)
    pad = -tiles % LANES
    outer_a = jnp.pad(outer_a, ((0, 0), (0, pad)))
    outer_b = jnp.pad(outer_b, ((0, 0), (0, pad)))
    return pl.pallas_call(
        table_kernel,
        out_shape=[jax.ShapeDtypeStruct((rows, length), BF16)] * 2,
        in_specs=vmem(4),
        out_specs=vmem(2),
        name="waves",
        cost_estimate=pl.CostEstimate(
            flops=rows * length * 8, bytes_accessed=rows * length * 4, transcendentals=0
        ),
    )(outer_a, outer_b, jnp.cos(near), jnp.sin(near))


def forward_kernel(radii, table, rest, surf, out):
    over_lanes = (((1,), (1,)), ((), ()))
    both = lax.dot_general(table[...], surf[...], over_lanes, preferred_element_type=F32)
    fine = lax.dot_general(rest[...], surf[:radii, :], over_lanes, preferred_element_type=F32)
    sums = both[:, :radii] + (both[:, radii:] + fine)
    row = lax.broadcasted_iota(jnp.int32, sums.shape, 0)
    sums = jnp.where(row == 0, sums + LEVELS[0] * surf.shape[1], sums)
    out[...] = sums.astype(BF16)


def forward(table, rest, surf):
    return pl.pallas_call(
        functools.partial(forward_kernel, surf.shape[0] // 2),
        out_shape=jax.ShapeDtypeStruct((table.shape[0], surf.shape[0] // 2), BF16),
        in_specs=vmem(3),
        out_specs=vmem(1)[0],
        name="forward",
    )(table, rest, surf)


def kick_kernel(radii, width, modes_ref, scale_ref, wave_ref, table, swept, out):
    length = table.shape[1]
    chunk = max(width, LANES)
    modes = modes_ref[...].astype(F32).T * scale_ref[...]
    size, rows = modes.shape
    radial = 0.5 * (pltpu.roll(modes, size - 2, 0)[:radii] - modes[:radii])
    potential = pltpu.roll(modes, size - 1, 0)[:radii]
    column = lax.broadcasted_iota(jnp.int32, potential.shape, 1)
    following, previous = pltpu.roll(potential, rows - 1, 1), pltpu.roll(potential, 1, 1)
    azimuthal = jnp.where(column % 2 == 0, -following, previous) * wave_ref[...]
    parts = []
    for x in (radial, azimuthal):
        parts.append(x.astype(BF16))
        parts.append((x - parts[-1].astype(F32)).astype(BF16))
    parts = jnp.concatenate(parts, axis=0)

    def one_chunk(i, carry):
        lanes = pl.ds(pl.multiple_of(i * chunk, LANES), chunk)
        slopes = jnp.dot(parts, table[:, lanes], preferred_element_type=F32)
        slope_r = slopes[:radii] + slopes[radii : 2 * radii]
        slope_az = slopes[2 * radii : 3 * radii] + slopes[3 * radii :]
        density = swept[0, :, lanes]
        values = (
            density,
            swept[1, :, lanes] - kick_radial * density * slope_r,
            swept[2, :, lanes] - kick_azimuth * density * slope_az,
            swept[3, :, lanes],
            swept[4, :, lanes],
        )
        for f in range(FIELDS):
            value = (values[f] - LEVELS[f]).astype(BF16)
            for k in range(chunk // width):
                out[i * (chunk // width) + k, f * radii : (f + 1) * radii, :] = value[
                    :, k * width : (k + 1) * width
                ]
        return carry

    lax.fori_loop(0, length // chunk, one_chunk, 0)


def kick(modes, table, swept, width):
    rows, length = table.shape
    radii = swept.shape[1]
    mode = jnp.arange(rows, dtype=jnp.int32)[None, :] // 2
    scale = jnp.where(mode == 0, 1.0, 2.0).astype(F32) / length
    wave = mode.astype(F32) * (2.0 * math.pi / length)
    return pl.pallas_call(
        functools.partial(kick_kernel, radii, width),
        out_shape=jax.ShapeDtypeStruct((length // width, FIELDS * radii, width), BF16),
        in_specs=vmem(5),
        out_specs=vmem(1)[0],
        name="kick",
    )(modes, scale, wave, table, swept)


def unpack_kernel(radii, got, *outs):
    per_tile = LANES // radii
    for f in range(FIELDS):
        rows = [got[k, f * radii : (f + 1) * radii, :].astype(F32) for k in range(per_tile)]
        outs[f][0] = jnp.concatenate(rows, axis=0).T + LEVELS[f]


def unpack(got, radii):
    sources, rows, width = got.shape
    total = sources * radii
    per_tile = LANES // radii
    return pl.pallas_call(
        functools.partial(unpack_kernel, radii),
        grid=(total // LANES,),
        out_shape=[jax.ShapeDtypeStruct((1, width, total), F32)] * FIELDS,
        in_specs=[pl.BlockSpec((per_tile, rows, width), lambda c: (c, 0, 0))],
        out_specs=[pl.BlockSpec((1, width, LANES), lambda c: (0, 0, c))] * FIELDS,
        name="unpack",
    )(got)


def exchange(x):
    return lax.all_to_all(x, "az", split_axis=0, concat_axis=0, tiled=True)


def shards(density, mom_radial, mom_azimuth, energy, dust, shifts, green):
    fields = (density, mom_radial, mom_azimuth, energy, dust)
    layers, width, total = density.shape
    devices = lax.axis_size("az")
    me = lax.axis_index("az")
    radii = total // devices
    length = width * devices
    modes_dev = green.shape[0]
    rows = 2 * modes_dev * devices
    assert layers == 1 and radii % 16 == 0 and LANES % radii == 0

    got = exchange(pack(fields, radii, devices))

    around = lax.dynamic_slice_in_dim(jnp.pad(shifts, (HALO, HALO), mode="edge"), me * radii, radii + 2 * HALO)
    amounts = jnp.concatenate(
        [around[HALO : HALO + radii], around[HALO + radii :], around[:HALO], jnp.zeros((8 - 2 * HALO,), jnp.int32)]
    )
    amounts = jnp.broadcast_to(amounts[:, None], (radii + 8, LANES))
    table, rest = waves(rows, length)

    swept, surf = sweeps(got, amounts, radii)
    coeffs = exchange(forward(table, rest, surf).reshape(devices, 2 * modes_dev, radii))
    coeffs = coeffs.transpose(1, 0, 2).reshape(modes_dev, 2, total)
    potential = jnp.einsum("mrs,mcs->mcr", green, coeffs, preferred_element_type=F32)
    potential = potential.astype(BF16).reshape(2 * modes_dev, total)
    padded = jnp.pad(potential, ((0, 0), (1, 1)), mode="edge")
    room = -(-(radii + 2) // LANES) * LANES
    windows = jnp.stack([padded[:, d * radii : (d + 1) * radii + 2] for d in range(devices)])
    windows = jnp.pad(windows, ((0, 0), (0, 0), (0, room - radii - 2)))
    modes = exchange(windows).reshape(rows, room)

    back = exchange(kick(modes, table, swept, width))
    return tuple(unpack(back, radii))


def solution(mesh):
    spec = P("groups", "az", None)
    return jax.shard_map(
        shards,
        mesh=mesh,
        in_specs=(spec,) * FIELDS + (P("groups"), P("az", None, None)),
        out_specs=(spec,) * FIELDS,
        check_vma=False,
    )
```

```python
import functools
import math

import jax
import jax.numpy as jnp
from jax import lax
from jax.experimental import pallas as pl
from jax.experimental.pallas import tpu as pltpu
from jax.sharding import PartitionSpec as P


courant = 0.05
kick_radial = 0.1
kick_azimuth = 3.0
FIELDS = 5
GAS = (0, 1, 2)
CARRIED = (3, 4)
LANES = 128
CHUNK = 1024
HALO = 2
HALO_ROWS = 16
RANGES = ((0.5, 2.0), (-3.0, 3.0), (-3.0, 3.0), (0.5, 2.0), (0.1, 1.0))
LEVELS = tuple(0.5 * (low + high) for low, high in RANGES)
STEPS = tuple(0.5 * (high - low) / 32760.0 for low, high in RANGES)
CODE = jnp.int16
BF16 = jnp.bfloat16
F32 = jnp.float32


def vmem(count):
    return [pl.BlockSpec(memory_space=pltpu.VMEM)] * count


HBM_SPEC = pl.BlockSpec(memory_space=pltpu.HBM)


def grant(mebibytes):
    return pltpu.CompilerParams(vmem_limit_bytes=mebibytes * 1024 * 1024)


def cost(flops):
    return pl.CostEstimate(flops=flops, bytes_accessed=0, transcendentals=0)


def pack_kernel(ids, radii, dests, *refs):
    count = len(ids)
    sources, out = refs[:count], refs[count]
    fields, halo, arrived = refs[count + 1 :]
    tiles = radii * dests // LANES
    per_tile = LANES // radii

    def copy(p, c):
        lanes = pl.ds(c * LANES, LANES)
        return pltpu.make_async_copy(
            sources[p].at[0, :, lanes], fields.at[p, :, lanes], arrived.at[p, c]
        )

    for c in range(tiles):
        for p in range(count):
            copy(p, c).start()
    for c in range(tiles):
        for p, f in enumerate(ids):
            copy(p, c).wait()
            block = fields[p, :, c * LANES : (c + 1) * LANES].T
            block = jnp.floor((block - LEVELS[f]) * (1.0 / STEPS[f]) + 0.5)
            for k in range(per_tile):
                dest = c * per_tile + k
                own = block[k * radii : (k + 1) * radii]
                out[dest, p * radii : (p + 1) * radii, :] = own.astype(jnp.int32).astype(CODE)
                first, last = own[:HALO], own[radii - HALO :]
                row = p * 2 * HALO
                if dest > 0:
                    halo[dest - 1, row : row + HALO, :] = first
                else:
                    for i in range(HALO):
                        halo[0, row + HALO + i : row + HALO + i + 1, :] = own[:1]
                if dest < dests - 1:
                    halo[dest + 1, row + HALO : row + 2 * HALO, :] = last
                else:
                    for i in range(HALO):
                        halo[dest, row + i : row + i + 1, :] = own[radii - 1 :]
    used = count * 2 * HALO
    for dest in range(dests):
        halo[dest, used:, :] = jnp.zeros((HALO_ROWS - used, halo.shape[2]), F32)
        out[dest, count * radii :, :] = halo[dest].astype(jnp.int32).astype(CODE)


def pack(fields, ids, radii, dests):
    width, total = fields[0].shape[1:]
    rows = len(ids) * radii + HALO_ROWS
    return pl.pallas_call(
        functools.partial(pack_kernel, ids, radii, dests),
        out_shape=jax.ShapeDtypeStruct((dests, rows, width), CODE),
        in_specs=[HBM_SPEC] * len(ids),
        out_specs=vmem(1)[0],
        scratch_shapes=[
            pltpu.VMEM((len(ids), width, total), F32),
            pltpu.VMEM((dests, HALO_ROWS, width), F32),
            pltpu.SemaphoreType.DMA((len(ids), total // LANES)),
        ],
        compiler_params=grant(60),
        cost_estimate=cost(20 * len(ids) * width * total),
        name="pack",
    )(*[fields[f] for f in ids])


def after(x, axis):
    return pltpu.roll(x, x.shape[axis] - 1, axis)


def before(x, axis):
    return pltpu.roll(x, 1, axis)


def limited(q, axis):
    following = after(q, axis)
    d = following - q
    bend = (before(d, axis) - after(d, axis)) * (1.0 / 12.0)
    half = 0.5 * d
    low, high = jnp.minimum(d, 0.0), jnp.maximum(d, 0.0)
    left = q + jnp.minimum(jnp.maximum(half + bend, low), high)
    right = following - jnp.minimum(jnp.maximum(half - bend, low), high)
    return left, right


def updated(q, flux, axis):
    return q - courant * (flux - before(flux, axis))


def gas_sweep(cells, axis, normal):
    states = [limited(q, axis) for q in cells]
    (left, right), (n_left, n_right) = states[0], states[normal]
    u_left, u_right = n_left / left, n_right / right
    speed = jnp.maximum(jnp.abs(u_left), jnp.abs(u_right)) + 1.0
    w_left, w_right = 0.5 * (u_left + speed), 0.5 * (u_right - speed)
    fluxes = [one * w_left + two * w_right for one, two in states]
    fluxes[normal] = fluxes[normal] + 0.5 * (left + right)
    return [updated(q, flux, axis) for q, flux in zip(cells, fluxes)], (w_left, w_right)


def carried_sweep(q, weights, axis):
    left, right = limited(q, axis)
    return updated(q, left * weights[0] + right * weights[1], axis)


def shifted_tiles(tiles, amount):
    count = len(tiles)
    fine, coarse = amount % LANES, amount // LANES
    lane = lax.broadcasted_iota(jnp.int32, amount.shape, 1)
    index = (lane - fine) % LANES
    wraps = lane < fine
    turned = [jnp.take_along_axis(x, index, axis=1, mode="promise_in_bounds") for x in tiles]
    tiles = [jnp.where(wraps, turned[t - 1], turned[t]) for t in range(count)]
    for bit in range((count - 1).bit_length()):
        chosen = (coarse >> bit) & 1 == 1
        tiles = [jnp.where(chosen, tiles[(t - (1 << bit)) % count], tiles[t]) for t in range(count)]
    return tiles


def decode(ids, radii, got, wide):
    sources, _, width = got.shape
    for p, f in enumerate(ids):
        for src in range(sources):
            lanes = slice(src * width, (src + 1) * width)
            codes = got[src, p * radii : (p + 1) * radii, :].astype(jnp.int32)
            wide[p, :radii, lanes] = codes.astype(F32) * STEPS[f] + LEVELS[f]
    for src in range(sources):
        lanes = slice(src * width, (src + 1) * width)
        edge = got[src, len(ids) * radii :, :].astype(jnp.int32).astype(F32)
        for p, f in enumerate(ids):
            own = edge[p * 2 * HALO : (p + 1) * 2 * HALO]
            wide[p, radii : radii + 2 * HALO, lanes] = own * STEPS[f] + LEVELS[f]
            wide[p, radii + 2 * HALO :, lanes] = jnp.ones((8 - 2 * HALO, width), F32)


def turn(count, rows, amount, wide, turned):
    tiles = wide.shape[2] // LANES

    def one_field(p, carry):
        out = shifted_tiles([wide[p, rows, t * LANES : (t + 1) * LANES] for t in range(tiles)], amount)
        for t in range(tiles):
            turned[p, :, (t + 1) * LANES : (t + 2) * LANES] = out[t]
        turned[p, :, :LANES] = out[tiles - 1]
        turned[p, :, (tiles + 1) * LANES :] = out[0]
        return carry

    lax.fori_loop(0, count, one_field, 0)


def place_lower_halo(count, radii, mid, lanes):
    for p in range(count):
        mid[p, 8 - HALO : 8, lanes] = mid[p, radii + 8 + HALO : radii + 8 + 2 * HALO, lanes]


def eight(b, offset=0):
    return pl.ds(pl.multiple_of(b * 8 + offset, 8), 8)


def gas_kernel(
    radii, chunk, got, amounts, table_hbm, rest_hbm, swept, coeffs, w_az, w_rad, wide, turned, mid, surf, table, rest, arrived
):
    count = len(GAS)
    length = wide.shape[2]
    copies = [
        pltpu.make_async_copy(source, dest, arrived.at[k])
        for k, (source, dest) in enumerate(((table_hbm, table), (rest_hbm, rest)))
    ]
    for copy in copies:
        copy.start()
    decode(GAS, radii, got, wide)

    def one_block(b, carry):
        turn(count, eight(b), amounts[eight(b), :], wide, turned)

        def one_chunk(i, carry):
            start = pl.multiple_of(i * chunk, LANES)
            cells = [turned[p, :, pl.ds(start, chunk + 2 * LANES)] for p in range(count)]
            out, weights = gas_sweep(cells, 1, 2)
            for p in range(count):
                mid[p, eight(b, 8), pl.ds(start, chunk)] = out[p][:, LANES : LANES + chunk]
            for k in range(2):
                w_az[k, eight(b), pl.ds(pl.multiple_of(start + LANES, LANES), chunk)] = weights[k][
                    :, LANES : LANES + chunk
                ]
            return carry

        lax.fori_loop(0, length // chunk, one_chunk, 0)
        for k in range(2):
            w_az[k, eight(b), :LANES] = w_az[k, eight(b), length : length + LANES]
            w_az[k, eight(b), length + LANES :] = jnp.zeros((8, LANES), F32)
        return carry

    lax.fori_loop(0, radii // 8 + 1, one_block, 0)

    def one_tile(t, carry):
        lanes = pl.ds(pl.multiple_of(t * LANES, LANES), LANES)
        place_lower_halo(count, radii, mid, lanes)
        out, weights = gas_sweep([mid[p, :, lanes] for p in range(count)], 0, 1)
        for p in range(count):
            swept[p, :, lanes] = out[p][8 : 8 + radii]
        for k in range(2):
            w_rad[k, :, lanes] = weights[k]
        ripple = out[0][8 : 8 + radii] - LEVELS[0]
        high = ripple.astype(BF16)
        surf[:radii, lanes] = high
        surf[radii:, lanes] = (ripple - high.astype(F32)).astype(BF16)
        return carry

    lax.fori_loop(0, length // LANES, one_tile, 0)

    for copy in copies:
        copy.wait()
    over_lanes = (((1,), (1,)), ((), ()))
    both = lax.dot_general(table[...], surf[...], over_lanes, preferred_element_type=F32)
    fine = lax.dot_general(rest[...], surf[:radii, :], over_lanes, preferred_element_type=F32)
    sums = both[:, :radii] + (both[:, radii:] + fine)
    row = lax.broadcasted_iota(jnp.int32, sums.shape, 0)
    sums = jnp.where(row == 0, sums + LEVELS[0] * length, sums)
    coeffs[:, :radii] = sums.astype(BF16)
    if coeffs.shape[1] > radii:
        coeffs[:, radii:] = jnp.zeros((coeffs.shape[0], coeffs.shape[1] - radii), BF16)


def scratches(count, radii, length):
    return [
        pltpu.VMEM((count, radii + 8, length), F32),
        pltpu.VMEM((count, 8, length + 2 * LANES), F32),
        pltpu.VMEM((count, radii + 16, length), F32),
    ]


def gas_sweeps(got, amounts, table, rest, radii):
    sources, _, width = got.shape
    length = sources * width
    return pl.pallas_call(
        functools.partial(gas_kernel, radii, min(CHUNK, length)),
        out_shape=(
            jax.ShapeDtypeStruct((len(GAS), radii, length), F32),
            jax.ShapeDtypeStruct((table.shape[0], LANES), BF16),
            jax.ShapeDtypeStruct((2, radii + 8, length + 2 * LANES), F32),
            jax.ShapeDtypeStruct((2, radii + 16, length), F32),
        ),
        in_specs=vmem(2) + [HBM_SPEC] * 2,
        out_specs=tuple(vmem(4)),
        scratch_shapes=scratches(len(GAS), radii, length)
        + [
            pltpu.VMEM((2 * radii, length), BF16),
            pltpu.VMEM(table.shape, BF16),
            pltpu.VMEM(table.shape, BF16),
            pltpu.SemaphoreType.DMA((2,)),
        ],
        compiler_params=grant(50),
        cost_estimate=cost(300 * radii * length),
        name="gas_sweeps",
    )(got, amounts, table, rest)


def carried_kernel(radii, chunk, got, amounts, w_az, w_rad, out, wide, turned, mid):
    count = len(CARRIED)
    length = wide.shape[2]
    width = got.shape[2]
    decode(CARRIED, radii, got, wide)

    def one_block(b, carry):
        turn(count, eight(b), amounts[eight(b), :], wide, turned)

        def one_chunk(i, carry):
            start = pl.multiple_of(i * chunk, LANES)
            window = pl.ds(start, chunk + 2 * LANES)
            weights = [w_az[k, eight(b), window] for k in range(2)]
            for p in range(count):
                value = carried_sweep(turned[p, :, window], weights, 1)
                mid[p, eight(b, 8), pl.ds(start, chunk)] = value[:, LANES : LANES + chunk]
            return carry

        lax.fori_loop(0, length // chunk, one_chunk, 0)
        return carry

    lax.fori_loop(0, radii // 8 + 1, one_block, 0)

    def one_tile(t, carry):
        lanes = pl.ds(pl.multiple_of(t * LANES, LANES), LANES)
        place_lower_halo(count, radii, mid, lanes)
        weights = [w_rad[k, :, lanes] for k in range(2)]
        for p, f in enumerate(CARRIED):
            value = carried_sweep(mid[p, :, lanes], weights, 0)[8 : 8 + radii] - LEVELS[f]
            value = value.astype(BF16)
            rows = slice(p * radii, (p + 1) * radii)
            if width >= LANES:
                per = width // LANES
                out[t // per, rows, pl.ds(pl.multiple_of(t % per * LANES, LANES), LANES)] = value
            else:
                for k in range(LANES // width):
                    out[t * (LANES // width) + k, rows, :] = value[:, k * width : (k + 1) * width]
        return carry

    lax.fori_loop(0, length // LANES, one_tile, 0)


def carried_sweeps(got, amounts, w_az, w_rad, radii):
    sources, _, width = got.shape
    length = sources * width
    return pl.pallas_call(
        functools.partial(carried_kernel, radii, min(CHUNK, length)),
        out_shape=jax.ShapeDtypeStruct((sources, len(CARRIED) * radii, width), BF16),
        in_specs=vmem(4),
        out_specs=vmem(1)[0],
        scratch_shapes=scratches(len(CARRIED), radii, length),
        compiler_params=grant(16),
        cost_estimate=cost(150 * radii * length),
        name="carried_sweeps",
    )(got, amounts, w_az, w_rad)


def table_kernel(outer_a, outer_b, inner_a, inner_b, out, rest):
    tiles = out.shape[1] // LANES

    def rows_at(i, carry):
        rows = pl.ds(pl.multiple_of(i * 16, 16), 16)
        a, b = inner_a[rows, :], inner_b[rows, :]
        oa, ob = outer_a[rows, :], outer_b[rows, :]
        for t in range(tiles):
            value = oa[:, t : t + 1] * a + ob[:, t : t + 1] * b
            lanes = slice(t * LANES, (t + 1) * LANES)
            high = value.astype(BF16)
            out[rows, lanes] = high
            rest[rows, lanes] = (value - high.astype(F32)).astype(BF16)
        return carry

    lax.fori_loop(0, out.shape[0] // 16, rows_at, 0)


def waves(rows, length):
    tiles = length // LANES
    row = jnp.arange(rows, dtype=jnp.int32)
    mode, odd = row // 2, (row % 2 == 1)[:, None]

    def angle(positions):
        phase = mode[:, None] * positions[None, :] % length
        return phase.astype(F32) * (2.0 * math.pi / length)

    far = angle(jnp.arange(tiles, dtype=jnp.int32) * LANES)
    near = angle(jnp.arange(LANES, dtype=jnp.int32))
    cos_far, sin_far = jnp.cos(far), jnp.sin(far)
    outer_a = jnp.where(odd, -sin_far, cos_far)
    outer_b = jnp.where(odd, -cos_far, -sin_far)
    pad = -tiles % LANES
    outer_a = jnp.pad(outer_a, ((0, 0), (0, pad)))
    outer_b = jnp.pad(outer_b, ((0, 0), (0, pad)))
    return pl.pallas_call(
        table_kernel,
        out_shape=[jax.ShapeDtypeStruct((rows, length), BF16)] * 2,
        in_specs=vmem(4),
        out_specs=vmem(2),
        compiler_params=grant(60),
        name="waves",
        cost_estimate=pl.CostEstimate(
            flops=rows * length * 8, bytes_accessed=rows * length * 4, transcendentals=0
        ),
    )(outer_a, outer_b, jnp.cos(near), jnp.sin(near))


def kick_kernel(radii, width, modes_ref, scale_ref, wave_ref, table, swept, out, parts):
    @pl.when(pl.program_id(0) == 0)
    def _():
        modes = modes_ref[...].astype(F32).T * scale_ref[...]
        size, rows = modes.shape
        radial = 0.5 * (pltpu.roll(modes, size - 2, 0)[:radii] - modes[:radii])
        potential = pltpu.roll(modes, size - 1, 0)[:radii]
        column = lax.broadcasted_iota(jnp.int32, potential.shape, 1)
        following, previous = pltpu.roll(potential, rows - 1, 1), pltpu.roll(potential, 1, 1)
        azimuthal = jnp.where(column % 2 == 0, -following, previous) * wave_ref[...]
        for i, x in enumerate((radial, azimuthal)):
            high = x.astype(BF16)
            parts[2 * i * radii : (2 * i + 1) * radii, :] = high
            parts[(2 * i + 1) * radii : (2 * i + 2) * radii, :] = (x - high.astype(F32)).astype(BF16)

    slopes = jnp.dot(parts[...], table[...], preferred_element_type=F32)
    slope_r = slopes[:radii] + slopes[radii : 2 * radii]
    slope_az = slopes[2 * radii : 3 * radii] + slopes[3 * radii :]
    density = swept[0]
    values = (
        density,
        swept[1] - kick_radial * density * slope_r,
        swept[2] - kick_azimuth * density * slope_az,
    )
    for p, f in enumerate(GAS):
        value = (values[p] - LEVELS[f]).astype(BF16)
        for k in range(out.shape[0]):
            out[k, p * radii : (p + 1) * radii, :] = value[:, k * width : (k + 1) * width]


def kick(modes, table, swept, width):
    rows, length = table.shape
    radii = swept.shape[1]
    chunk = max(2 * width, LANES)
    mode = jnp.arange(rows, dtype=jnp.int32)[None, :] // 2
    scale = jnp.where(mode == 0, 1.0, 2.0).astype(F32) / length
    wave = mode.astype(F32) * (2.0 * math.pi / length)

    def whole(x):
        return pl.BlockSpec(x.shape, lambda i: (0, 0))

    return pl.pallas_call(
        functools.partial(kick_kernel, radii, width),
        grid=(length // chunk,),
        out_shape=jax.ShapeDtypeStruct((length // width, len(GAS) * radii, width), BF16),
        in_specs=[
            whole(modes),
            whole(scale),
            whole(wave),
            pl.BlockSpec((rows, chunk), lambda i: (0, i)),
            pl.BlockSpec((len(GAS), radii, chunk), lambda i: (0, 0, i)),
        ],
        out_specs=pl.BlockSpec((chunk // width, len(GAS) * radii, width), lambda i: (i, 0, 0)),
        scratch_shapes=[pltpu.VMEM((4 * radii, rows), BF16)],
        compiler_params=grant(58),
        cost_estimate=cost(16 * radii * rows * length),
        name="kick",
    )(modes, scale, wave, table, swept)


def unpack_kernel(ids, radii, got, *outs):
    per_tile = LANES // radii
    for p, f in enumerate(ids):
        rows = [got[k, p * radii : (p + 1) * radii, :].astype(F32) for k in range(per_tile)]
        outs[p][0] = jnp.concatenate(rows, axis=0).T + LEVELS[f]


def unpack(got, ids, radii):
    sources, rows, width = got.shape
    total = sources * radii
    per_tile = LANES // radii
    return pl.pallas_call(
        functools.partial(unpack_kernel, ids, radii),
        grid=(total // LANES,),
        out_shape=[jax.ShapeDtypeStruct((1, width, total), F32)] * len(ids),
        in_specs=[pl.BlockSpec((per_tile, rows, width), lambda c: (c, 0, 0))],
        out_specs=[pl.BlockSpec((1, width, LANES), lambda c: (0, 0, c))] * len(ids),
        compiler_params=grant(8),
        cost_estimate=cost(20 * len(ids) * width * total),
        name="unpack",
    )(got)


def exchange(x):
    return lax.all_to_all(x, "az", split_axis=0, concat_axis=0, tiled=True)


def shards(density, mom_radial, mom_azimuth, energy, dust, shifts, green):
    fields = (density, mom_radial, mom_azimuth, energy, dust)
    layers, width, total = density.shape
    devices = lax.axis_size("az")
    me = lax.axis_index("az")
    radii = total // devices
    length = width * devices
    modes_dev = green.shape[0]
    rows = 2 * modes_dev * devices
    assert layers == 1 and radii % 16 == 0 and LANES % radii == 0

    gas = exchange(pack(fields, GAS, radii, devices))
    gas, carried = lax.optimization_barrier((gas, pack(fields, CARRIED, radii, devices)))
    carried = exchange(carried)

    around = lax.dynamic_slice_in_dim(jnp.pad(shifts, (HALO, HALO), mode="edge"), me * radii, radii + 2 * HALO)
    amounts = jnp.concatenate(
        [around[HALO : HALO + radii], around[HALO + radii :], around[:HALO], jnp.zeros((8 - 2 * HALO,), jnp.int32)]
    )
    amounts = jnp.broadcast_to(amounts[:, None], (radii + 8, LANES))
    table, rest = waves(rows, length)

    swept, coeffs, w_az, w_rad = gas_sweeps(gas, amounts, table, rest, radii)
    coeffs = coeffs.reshape(devices, 2 * modes_dev, LANES)
    coeffs, carried = lax.optimization_barrier((coeffs, carried))
    coeffs = exchange(coeffs)[..., :radii]
    carried = carried_sweeps(carried, amounts, w_az, w_rad, radii)
    coeffs, carried = lax.optimization_barrier((coeffs, carried))
    back = exchange(carried)
    coeffs = coeffs.transpose(1, 0, 2).reshape(modes_dev, 2, total)
    potential = jnp.einsum("mrs,mcs->mcr", green, coeffs, preferred_element_type=F32)
    potential = potential.astype(BF16).reshape(2 * modes_dev, total)
    padded = jnp.pad(potential, ((0, 0), (1, 1)), mode="edge")
    room = -(-(radii + 2) // LANES) * LANES
    windows = jnp.stack([padded[:, d * radii : (d + 1) * radii + 2] for d in range(devices)])
    windows = jnp.pad(windows, ((0, 0), (0, 0), (0, room - radii - 2)))
    windows, back = lax.optimization_barrier((windows, back))
    modes = exchange(windows).reshape(rows, room)

    kicked = exchange(kick(modes, table, swept, width))
    return tuple(unpack(kicked, GAS, radii)) + tuple(unpack(back, CARRIED, radii))


def solution(mesh):
    spec = P("groups", "az", None)
    return jax.shard_map(
        shards,
        mesh=mesh,
        in_specs=(spec,) * FIELDS + (P("groups"), P("az", None, None)),
        out_specs=(spec,) * FIELDS,
        check_vma=False,
    )
```

```python
import functools
import math

import jax
import jax.numpy as jnp
from jax import lax
from jax.experimental import pallas as pl
from jax.experimental.pallas import tpu as pltpu
from jax.sharding import PartitionSpec as P


courant = 0.05
kick_radial = 0.1
kick_azimuth = 3.0
FIELDS = 5
GAS = (0, 1, 2)
CARRIED = (3, 4)
LANES = 128
CHUNK = 4096
HALO = 2
HALO_ROWS = 16
RANGES = ((0.5, 2.0), (-3.0, 3.0), (-3.0, 3.0), (0.5, 2.0), (0.1, 1.0))
LEVELS = tuple(0.5 * (low + high) for low, high in RANGES)
STEPS = tuple(0.5 * (high - low) / 32760.0 for low, high in RANGES)
CODE = jnp.int16
BF16 = jnp.bfloat16
F32 = jnp.float32


def vmem(count):
    return [pl.BlockSpec(memory_space=pltpu.VMEM)] * count


HBM_SPEC = pl.BlockSpec(memory_space=pltpu.HBM)


def grant(mebibytes):
    return pltpu.CompilerParams(vmem_limit_bytes=mebibytes * 1024 * 1024)


def cost(flops):
    return pl.CostEstimate(flops=flops, bytes_accessed=0, transcendentals=0)


def pack_kernel(ids, radii, dests, *refs):
    count = len(ids)
    sources, out = refs[:count], refs[count]
    fields, halo, arrived = refs[count + 1 :]
    tiles = radii * dests // LANES
    per_tile = LANES // radii

    def copy(p, c):
        lanes = pl.ds(c * LANES, LANES)
        return pltpu.make_async_copy(
            sources[p].at[0, :, lanes], fields.at[p, :, lanes], arrived.at[p, c]
        )

    for c in range(tiles):
        for p in range(count):
            copy(p, c).start()
    for c in range(tiles):
        for p, f in enumerate(ids):
            copy(p, c).wait()
            block = fields[p, :, c * LANES : (c + 1) * LANES].T
            block = jnp.floor((block - LEVELS[f]) * (1.0 / STEPS[f]) + 0.5)
            for k in range(per_tile):
                dest = c * per_tile + k
                own = block[k * radii : (k + 1) * radii]
                out[dest, p * radii : (p + 1) * radii, :] = own.astype(jnp.int32).astype(CODE)
                first, last = own[:HALO], own[radii - HALO :]
                row = p * 2 * HALO
                if dest > 0:
                    halo[dest - 1, row : row + HALO, :] = first
                else:
                    for i in range(HALO):
                        halo[0, row + HALO + i : row + HALO + i + 1, :] = own[:1]
                if dest < dests - 1:
                    halo[dest + 1, row + HALO : row + 2 * HALO, :] = last
                else:
                    for i in range(HALO):
                        halo[dest, row + i : row + i + 1, :] = own[radii - 1 :]
    used = count * 2 * HALO
    for dest in range(dests):
        halo[dest, used:, :] = jnp.zeros((HALO_ROWS - used, halo.shape[2]), F32)
        out[dest, count * radii :, :] = halo[dest].astype(jnp.int32).astype(CODE)


def pack(fields, ids, radii, dests):
    width, total = fields[0].shape[1:]
    rows = len(ids) * radii + HALO_ROWS
    return pl.pallas_call(
        functools.partial(pack_kernel, ids, radii, dests),
        out_shape=jax.ShapeDtypeStruct((dests, rows, width), CODE),
        in_specs=[HBM_SPEC] * len(ids),
        out_specs=vmem(1)[0],
        scratch_shapes=[
            pltpu.VMEM((len(ids), width, total), F32),
            pltpu.VMEM((dests, HALO_ROWS, width), F32),
            pltpu.SemaphoreType.DMA((len(ids), total // LANES)),
        ],
        compiler_params=grant(60),
        cost_estimate=cost(20 * len(ids) * width * total),
        name="pack",
    )(*[fields[f] for f in ids])


def after(x, axis):
    return pltpu.roll(x, x.shape[axis] - 1, axis)


def before(x, axis):
    return pltpu.roll(x, 1, axis)


def limited(q, axis):
    following = after(q, axis)
    d = following - q
    bend = (before(d, axis) - after(d, axis)) * (1.0 / 12.0)
    half = 0.5 * d
    low, high = jnp.minimum(d, 0.0), jnp.maximum(d, 0.0)
    left = q + jnp.minimum(jnp.maximum(half + bend, low), high)
    right = following - jnp.minimum(jnp.maximum(half - bend, low), high)
    return left, right


def updated(q, flux, axis):
    return q - courant * (flux - before(flux, axis))


def gas_sweep(cells, axis, normal):
    states = [limited(q, axis) for q in cells]
    (left, right), (n_left, n_right) = states[0], states[normal]
    u_left, u_right = n_left / left, n_right / right
    speed = jnp.maximum(jnp.abs(u_left), jnp.abs(u_right)) + 1.0
    w_left, w_right = 0.5 * (u_left + speed), 0.5 * (u_right - speed)
    fluxes = [one * w_left + two * w_right for one, two in states]
    fluxes[normal] = fluxes[normal] + 0.5 * (left + right)
    return [updated(q, flux, axis) for q, flux in zip(cells, fluxes)], (w_left, w_right)


def carried_sweep(q, weights, axis):
    left, right = limited(q, axis)
    return updated(q, left * weights[0] + right * weights[1], axis)


def shifted_tiles(tiles, amount):
    count = len(tiles)
    fine, coarse = amount % LANES, amount // LANES
    lane = lax.broadcasted_iota(jnp.int32, amount.shape, 1)
    index = (lane - fine) % LANES
    wraps = lane < fine
    turned = [jnp.take_along_axis(x, index, axis=1, mode="promise_in_bounds") for x in tiles]
    tiles = [jnp.where(wraps, turned[t - 1], turned[t]) for t in range(count)]
    for bit in range((count - 1).bit_length()):
        chosen = (coarse >> bit) & 1 == 1
        tiles = [jnp.where(chosen, tiles[(t - (1 << bit)) % count], tiles[t]) for t in range(count)]
    return tiles


def decode(ids, radii, got, wide):
    sources, _, width = got.shape
    for p, f in enumerate(ids):
        for src in range(sources):
            lanes = slice(src * width, (src + 1) * width)
            codes = got[src, p * radii : (p + 1) * radii, :].astype(jnp.int32)
            wide[p, :radii, lanes] = codes.astype(F32) * STEPS[f] + LEVELS[f]
    for src in range(sources):
        lanes = slice(src * width, (src + 1) * width)
        edge = got[src, len(ids) * radii :, :].astype(jnp.int32).astype(F32)
        for p, f in enumerate(ids):
            own = edge[p * 2 * HALO : (p + 1) * 2 * HALO]
            wide[p, radii : radii + 2 * HALO, lanes] = own * STEPS[f] + LEVELS[f]
            wide[p, radii + 2 * HALO :, lanes] = jnp.ones((8 - 2 * HALO, width), F32)


def turn(count, rows, amount, wide, turned):
    tiles = wide.shape[2] // LANES - 1

    def one_field(p, carry):
        out = shifted_tiles([wide[p, rows, t * LANES : (t + 1) * LANES] for t in range(tiles)], amount)
        for t in range(tiles):
            turned[p, :, (t + 1) * LANES : (t + 2) * LANES] = out[t]
        turned[p, :, :LANES] = out[tiles - 1]
        turned[p, :, (tiles + 1) * LANES :] = out[0]
        return carry

    lax.fori_loop(0, count, one_field, 0)


def place_lower_halo(count, radii, mid, lanes):
    for p in range(count):
        mid[p, 8 - HALO : 8, lanes] = mid[p, radii + 8 + HALO : radii + 8 + 2 * HALO, lanes]


def eight(b, offset=0):
    return pl.ds(pl.multiple_of(b * 8 + offset, 8), 8)


def gas_kernel(
    radii, chunk, got, amounts, table_hbm, rest_hbm, swept, coeffs, w_az, w_rad, wide, turned, mid, surf, table, rest, arrived
):
    count = len(GAS)
    length = wide.shape[2] - LANES
    copies = [
        pltpu.make_async_copy(source, dest, arrived.at[k])
        for k, (source, dest) in enumerate(((table_hbm, table), (rest_hbm, rest)))
    ]
    for copy in copies:
        copy.start()
    decode(GAS, radii, got, wide)

    def one_block(b, carry):
        turn(count, eight(b), amounts[eight(b), :], wide, turned)

        def one_chunk(i, carry):
            start = pl.multiple_of(i * chunk, LANES)
            cells = [turned[p, :, pl.ds(start, chunk + 2 * LANES)] for p in range(count)]
            out, weights = gas_sweep(cells, 1, 2)
            for p in range(count):
                mid[p, eight(b, 8), pl.ds(start, chunk)] = out[p][:, LANES : LANES + chunk]
            for k in range(2):
                w_az[k, eight(b), pl.ds(pl.multiple_of(start + LANES, LANES), chunk)] = weights[k][
                    :, LANES : LANES + chunk
                ]
            return carry

        lax.fori_loop(0, length // chunk, one_chunk, 0)
        for k in range(2):
            w_az[k, eight(b), :LANES] = w_az[k, eight(b), length : length + LANES]
            w_az[k, eight(b), length + LANES :] = jnp.zeros((8, LANES), F32)
        return carry

    lax.fori_loop(0, radii // 8 + 1, one_block, 0)

    def one_tile(t, carry):
        lanes = pl.ds(pl.multiple_of(t * LANES, LANES), LANES)
        place_lower_halo(count, radii, mid, lanes)
        out, weights = gas_sweep([mid[p, :, lanes] for p in range(count)], 0, 1)
        for p in range(count):
            swept[p, :, lanes] = out[p][8 : 8 + radii]
        for k in range(2):
            w_rad[k, :, lanes] = weights[k]
        ripple = out[0][8 : 8 + radii] - LEVELS[0]
        high = ripple.astype(BF16)
        surf[:radii, lanes] = high
        surf[radii:, lanes] = (ripple - high.astype(F32)).astype(BF16)
        return carry

    lax.fori_loop(0, length // LANES, one_tile, 0)

    for copy in copies:
        copy.wait()
    over_lanes = (((1,), (1,)), ((), ()))
    both = lax.dot_general(table[...], surf[...], over_lanes, preferred_element_type=F32)
    fine = lax.dot_general(rest[...], surf[:radii, :], over_lanes, preferred_element_type=F32)
    sums = both[:, :radii] + (both[:, radii:] + fine)
    row = lax.broadcasted_iota(jnp.int32, sums.shape, 0)
    sums = jnp.where(row == 0, sums + LEVELS[0] * length, sums)
    coeffs[:, :radii] = sums.astype(BF16)
    if coeffs.shape[1] > radii:
        coeffs[:, radii:] = jnp.zeros((coeffs.shape[0], coeffs.shape[1] - radii), BF16)


def scratches(count, radii, length):
    return [
        pltpu.VMEM((count, radii + 8, length + LANES), F32),
        pltpu.VMEM((count, 8, length + 2 * LANES), F32),
        pltpu.VMEM((count, radii + 16, length + LANES), F32),
    ]


def gas_sweeps(got, amounts, table, rest, radii):
    sources, _, width = got.shape
    length = sources * width
    return pl.pallas_call(
        functools.partial(gas_kernel, radii, min(CHUNK, length)),
        out_shape=(
            jax.ShapeDtypeStruct((len(GAS), radii, length), F32),
            jax.ShapeDtypeStruct((table.shape[0], LANES), BF16),
            jax.ShapeDtypeStruct((2, radii + 8, length + 2 * LANES), F32),
            jax.ShapeDtypeStruct((2, radii + 16, length + LANES), F32),
        ),
        in_specs=vmem(2) + [HBM_SPEC] * 2,
        out_specs=tuple(vmem(4)),
        scratch_shapes=scratches(len(GAS), radii, length)
        + [
            pltpu.VMEM((2 * radii, length), BF16),
            pltpu.VMEM(table.shape, BF16),
            pltpu.VMEM(table.shape, BF16),
            pltpu.SemaphoreType.DMA((2,)),
        ],
        compiler_params=grant(50),
        cost_estimate=cost(300 * radii * length),
        name="gas_sweeps",
    )(got, amounts, table, rest)


def carried_kernel(radii, chunk, got, amounts, w_az, w_rad, out, wide, turned, mid):
    count = len(CARRIED)
    length = wide.shape[2] - LANES
    width = got.shape[2]
    decode(CARRIED, radii, got, wide)

    def one_block(b, carry):
        turn(count, eight(b), amounts[eight(b), :], wide, turned)

        def one_chunk(i, carry):
            start = pl.multiple_of(i * chunk, LANES)
            window = pl.ds(start, chunk + 2 * LANES)
            weights = [w_az[k, eight(b), window] for k in range(2)]
            for p in range(count):
                value = carried_sweep(turned[p, :, window], weights, 1)
                mid[p, eight(b, 8), pl.ds(start, chunk)] = value[:, LANES : LANES + chunk]
            return carry

        lax.fori_loop(0, length // chunk, one_chunk, 0)
        return carry

    lax.fori_loop(0, radii // 8 + 1, one_block, 0)

    def one_tile(t, carry):
        lanes = pl.ds(pl.multiple_of(t * LANES, LANES), LANES)
        place_lower_halo(count, radii, mid, lanes)
        weights = [w_rad[k, :, lanes] for k in range(2)]
        for p, f in enumerate(CARRIED):
            value = carried_sweep(mid[p, :, lanes], weights, 0)[8 : 8 + radii] - LEVELS[f]
            value = value.astype(BF16)
            rows = slice(p * radii, (p + 1) * radii)
            if width >= LANES:
                per = width // LANES
                out[t // per, rows, pl.ds(pl.multiple_of(t % per * LANES, LANES), LANES)] = value
            else:
                for k in range(LANES // width):
                    out[t * (LANES // width) + k, rows, :] = value[:, k * width : (k + 1) * width]
        return carry

    lax.fori_loop(0, length // LANES, one_tile, 0)


def carried_sweeps(got, amounts, w_az, w_rad, radii):
    sources, _, width = got.shape
    length = sources * width
    return pl.pallas_call(
        functools.partial(carried_kernel, radii, min(CHUNK, length)),
        out_shape=jax.ShapeDtypeStruct((sources, len(CARRIED) * radii, width), BF16),
        in_specs=vmem(4),
        out_specs=vmem(1)[0],
        scratch_shapes=scratches(len(CARRIED), radii, length),
        compiler_params=grant(60),
        cost_estimate=cost(150 * radii * length),
        name="carried_sweeps",
    )(got, amounts, w_az, w_rad)


def table_kernel(outer_a, outer_b, inner_a, inner_b, out, rest):
    tiles = out.shape[1] // LANES

    def rows_at(i, carry):
        rows = pl.ds(pl.multiple_of(i * 16, 16), 16)
        a, b = inner_a[rows, :], inner_b[rows, :]
        oa, ob = outer_a[rows, :], outer_b[rows, :]
        for t in range(tiles):
            value = oa[:, t : t + 1] * a + ob[:, t : t + 1] * b
            lanes = slice(t * LANES, (t + 1) * LANES)
            high = value.astype(BF16)
            out[rows, lanes] = high
            rest[rows, lanes] = (value - high.astype(F32)).astype(BF16)
        return carry

    lax.fori_loop(0, out.shape[0] // 16, rows_at, 0)


def waves(rows, length):
    tiles = length // LANES
    row = jnp.arange(rows, dtype=jnp.int32)
    mode, odd = row // 2, (row % 2 == 1)[:, None]

    def angle(positions):
        phase = mode[:, None] * positions[None, :] % length
        return phase.astype(F32) * (2.0 * math.pi / length)

    far = angle(jnp.arange(tiles, dtype=jnp.int32) * LANES)
    near = angle(jnp.arange(LANES, dtype=jnp.int32))
    cos_far, sin_far = jnp.cos(far), jnp.sin(far)
    outer_a = jnp.where(odd, -sin_far, cos_far)
    outer_b = jnp.where(odd, -cos_far, -sin_far)
    pad = -tiles % LANES
    outer_a = jnp.pad(outer_a, ((0, 0), (0, pad)))
    outer_b = jnp.pad(outer_b, ((0, 0), (0, pad)))
    return pl.pallas_call(
        table_kernel,
        out_shape=[jax.ShapeDtypeStruct((rows, length), BF16)] * 2,
        in_specs=vmem(4),
        out_specs=vmem(2),
        compiler_params=grant(60),
        name="waves",
        cost_estimate=pl.CostEstimate(
            flops=rows * length * 8, bytes_accessed=rows * length * 4, transcendentals=0
        ),
    )(outer_a, outer_b, jnp.cos(near), jnp.sin(near))


def kick_kernel(radii, width, modes_ref, scale_ref, wave_ref, table, swept, out, parts):
    @pl.when(pl.program_id(0) == 0)
    def _():
        modes = modes_ref[...].astype(F32).T * scale_ref[...]
        size, rows = modes.shape
        radial = 0.5 * (pltpu.roll(modes, size - 2, 0)[:radii] - modes[:radii])
        potential = pltpu.roll(modes, size - 1, 0)[:radii]
        column = lax.broadcasted_iota(jnp.int32, potential.shape, 1)
        following, previous = pltpu.roll(potential, rows - 1, 1), pltpu.roll(potential, 1, 1)
        azimuthal = jnp.where(column % 2 == 0, -following, previous) * wave_ref[...]
        for i, x in enumerate((radial, azimuthal)):
            high = x.astype(BF16)
            parts[2 * i * radii : (2 * i + 1) * radii, :] = high
            parts[(2 * i + 1) * radii : (2 * i + 2) * radii, :] = (x - high.astype(F32)).astype(BF16)

    slopes = jnp.dot(parts[...], table[...], preferred_element_type=F32)
    slope_r = slopes[:radii] + slopes[radii : 2 * radii]
    slope_az = slopes[2 * radii : 3 * radii] + slopes[3 * radii :]
    density = swept[0]
    values = (
        density,
        swept[1] - kick_radial * density * slope_r,
        swept[2] - kick_azimuth * density * slope_az,
    )
    for p, f in enumerate(GAS):
        value = (values[p] - LEVELS[f]).astype(BF16)
        for k in range(out.shape[0]):
            out[k, p * radii : (p + 1) * radii, :] = value[:, k * width : (k + 1) * width]


def kick(modes, table, swept, width):
    rows, length = table.shape
    radii = swept.shape[1]
    chunk = max(2 * width, LANES)
    mode = jnp.arange(rows, dtype=jnp.int32)[None, :] // 2
    scale = jnp.where(mode == 0, 1.0, 2.0).astype(F32) / length
    wave = mode.astype(F32) * (2.0 * math.pi / length)

    def whole(x):
        return pl.BlockSpec(x.shape, lambda i: (0, 0))

    return pl.pallas_call(
        functools.partial(kick_kernel, radii, width),
        grid=(length // chunk,),
        out_shape=jax.ShapeDtypeStruct((length // width, len(GAS) * radii, width), BF16),
        in_specs=[
            whole(modes),
            whole(scale),
            whole(wave),
            pl.BlockSpec((rows, chunk), lambda i: (0, i)),
            pl.BlockSpec((len(GAS), radii, chunk), lambda i: (0, 0, i)),
        ],
        out_specs=pl.BlockSpec((chunk // width, len(GAS) * radii, width), lambda i: (i, 0, 0)),
        scratch_shapes=[pltpu.VMEM((4 * radii, rows), BF16)],
        compiler_params=grant(58),
        cost_estimate=cost(16 * radii * rows * length),
        name="kick",
    )(modes, scale, wave, table, swept)


def unpack_kernel(ids, radii, got, *outs):
    per_tile = LANES // radii
    for p, f in enumerate(ids):
        rows = [got[k, p * radii : (p + 1) * radii, :].astype(F32) for k in range(per_tile)]
        outs[p][0] = jnp.concatenate(rows, axis=0).T + LEVELS[f]


def unpack(got, ids, radii):
    sources, rows, width = got.shape
    total = sources * radii
    per_tile = LANES // radii
    return pl.pallas_call(
        functools.partial(unpack_kernel, ids, radii),
        grid=(total // LANES,),
        out_shape=[jax.ShapeDtypeStruct((1, width, total), F32)] * len(ids),
        in_specs=[pl.BlockSpec((per_tile, rows, width), lambda c: (c, 0, 0))],
        out_specs=[pl.BlockSpec((1, width, LANES), lambda c: (0, 0, c))] * len(ids),
        compiler_params=grant(8),
        cost_estimate=cost(20 * len(ids) * width * total),
        name="unpack",
    )(got)


def exchange(x):
    return lax.all_to_all(x, "az", split_axis=0, concat_axis=0, tiled=True)


def shards(density, mom_radial, mom_azimuth, energy, dust, shifts, green):
    fields = (density, mom_radial, mom_azimuth, energy, dust)
    layers, width, total = density.shape
    devices = lax.axis_size("az")
    me = lax.axis_index("az")
    radii = total // devices
    length = width * devices
    modes_dev = green.shape[0]
    rows = 2 * modes_dev * devices
    assert layers == 1 and radii % 16 == 0 and LANES % radii == 0

    gas = exchange(pack(fields, GAS, radii, devices))
    gas, carried = lax.optimization_barrier((gas, pack(fields, CARRIED, radii, devices)))
    carried = exchange(carried)

    around = lax.dynamic_slice_in_dim(jnp.pad(shifts, (HALO, HALO), mode="edge"), me * radii, radii + 2 * HALO)
    amounts = jnp.concatenate(
        [around[HALO : HALO + radii], around[HALO + radii :], around[:HALO], jnp.zeros((8 - 2 * HALO,), jnp.int32)]
    )
    amounts = jnp.broadcast_to(amounts[:, None], (radii + 8, LANES))
    table, rest = waves(rows, length)

    swept, coeffs, w_az, w_rad = gas_sweeps(gas, amounts, table, rest, radii)
    coeffs = coeffs.reshape(devices, 2 * modes_dev, LANES)
    coeffs, carried = lax.optimization_barrier((coeffs, carried))
    coeffs = exchange(coeffs)[..., :radii]
    carried = carried_sweeps(carried, amounts, w_az, w_rad, radii)
    coeffs, carried = lax.optimization_barrier((coeffs, carried))
    back = exchange(carried)
    coeffs = coeffs.transpose(1, 0, 2).reshape(modes_dev, 2, total)
    potential = jnp.einsum("mrs,mcs->mcr", green, coeffs, preferred_element_type=F32)
    potential = potential.astype(BF16).reshape(2 * modes_dev, total)
    padded = jnp.pad(potential, ((0, 0), (1, 1)), mode="edge")
    room = -(-(radii + 2) // LANES) * LANES
    windows = jnp.stack([padded[:, d * radii : (d + 1) * radii + 2] for d in range(devices)])
    windows = jnp.pad(windows, ((0, 0), (0, 0), (0, room - radii - 2)))
    windows, back = lax.optimization_barrier((windows, back))
    modes = exchange(windows).reshape(rows, room)

    kicked = exchange(kick(modes, table, swept, width))
    return tuple(unpack(kicked, GAS, radii)) + tuple(unpack(back, CARRIED, radii))


def solution(mesh):
    spec = P("groups", "az", None)
    return jax.shard_map(
        shards,
        mesh=mesh,
        in_specs=(spec,) * FIELDS + (P("groups"), P("az", None, None)),
        out_specs=(spec,) * FIELDS,
        check_vma=False,
    )
```
